256 devices in a mesh: dp: 64 (over x, z, core), mp: 4 (over y).
Axes of the slice: x: 4, y: 4, z: 8, core: 2. Of those that a mesh axis runs over, the one named last changes fastest.
Arguments:
- sparse_vecs: bfloat16 [65536, 26, 128], P(('dp', 'mp')), may hold values from -6 to 6
- dense_vec: bfloat16 [65536, 128], P(('dp', 'mp')), may hold values from -6 to 6
- top_cot: bfloat16 [65536, 1024], P(('dp', 'mp')), may hold values from -0.59765625 to 0.59765625
- top_weight: bfloat16 [479, 1024], replicated, may hold values from -0.25 to 0.25
- owner_ids: int32 [65536, 26, 1], P(('dp', 'mp')), may hold values from 0 to 63; in each aligned block of 6656 rows (0 to 6655, 6656 to 13311, ..., all dimensions but the last counted through in order) at most 208 rows name the same one
- local_rows: int32 [65536, 26], P(('dp', 'mp')), may hold values from 0 to 127
- table: float32 [26, 8192, 128], P(None, ('dp', 'mp')), may hold values from -0.6 to 0.6
- accum: float32 [26, 8192], P(None, ('dp', 'mp')), may hold values from 0.05 to 2
Outputs:
- dense_grad: bfloat16 [65536, 128], P(('dp', 'mp'))
- new_table: float32 [26, 8192, 128], P(None, ('dp', 'mp'))
- new_accum: float32 [26, 8192], P(None, ('dp', 'mp'))
The draws below stay inside these ranges and needn't reach their ends.
Inputs may be any that keep to these rules, and one draw needn't show every extreme that they name: `owner_ids`: among the lookups of one device's 256 samples no owner group is named more than 208 times; in every draw some device names some owner group exactly 208 times.
All inputs are finite; a program needn't handle non-finite values.
Results may differ from the reference program's by a relative error of at most 0.005.
Values may be sent and summed in bfloat16 or wider, within the bound.
A program may use at most 128 MiB of HBM per device.

```python
import math
import jax
import jax.numpy as jnp
import numpy as np
from jax import lax

E = 128
TABLES = 26
H1 = 1024
B_DEV = 256
ZIN = 479
BATCH = 65536
LOOK_DEV = 6656
ROWS_GRP = 128
ROWS = 8192
CAP = 208
N_DP = 64


def with_ends(drawn, rng, low, high):
    place = [jax.random.randint(jax.random.fold_in(rng, axis), (), 0, length) for axis, length in enumerate(drawn.shape)]
    main_axis = drawn.shape.index(max(drawn.shape))
    next_to = place[:main_axis] + [(place[main_axis] + 1) % drawn.shape[main_axis]] + place[main_axis + 1:]
    return drawn.at[tuple(place)].set(low).at[tuple(next_to)].set(high)


def shard_levels(key, extent, pieces, low, largest):
    def one(axis_at, shards_of):
        steps = jax.random.uniform(jax.random.fold_in(jax.random.fold_in(key, 6), axis_at), (shards_of,), jnp.float32, low / len(pieces), largest / len(pieces))
        return jnp.repeat(jnp.exp(steps), extent[axis_at] // shards_of).reshape((-1,) + (1,) * (len(extent) - axis_at - 1))

    gain = one(*pieces[0])
    for cut in pieces[1:]:
        gain = gain * one(*cut)
    return gain


def rank_bounds(count, lean):
    loads = [(1 << 20) // math.isqrt(standing ** lean) + 1 for standing in range(1, count + 1)]
    spread = 1 + sum(loads) // (1 << 30)
    return np.cumsum(np.array([max(1, weight // spread) for weight in loads]))


def ranked(key, dims, amount, lean):
    listing = rank_bounds(amount, lean)
    ticket = jax.random.randint(jax.random.fold_in(key, 1), dims, 0, int(listing[amount - 1]))
    standing = jnp.searchsorted(jnp.asarray(listing, jnp.int32), ticket, side="right")
    return jax.random.permutation(jax.random.fold_in(key, 2), amount)[standing].astype(jnp.int32)


def shared_out(own_key, own, number, rows, number_of, top, most, slope):
    order = jax.random.permutation(own_key, number_of)
    heavy_load, usual = load_shares(number_of, rows * top, most, slope, True), load_shares(number_of, rows * top, most, slope, False)
    places = jnp.arange(number_of)

    def named(sizes, rotation):
        used = int((sizes > 0).sum())
        fixed = max(1, used // 4)
        moved = fixed + (places - fixed + rotation * (used - fixed)) % max(1, number_of - fixed)
        return jnp.zeros((number_of,), jnp.int32).at[order[jnp.where(places < fixed, places, moved)]].set(jnp.asarray(sizes, jnp.int32))

    sizes = jnp.where(number % 4 == 0, named(heavy_load, number // 4), named(usual, number - number // 4 - 1))
    mixed = jax.random.permutation(jax.random.fold_in(own, 3), number_of)
    donor, taker = mixed[0:number_of // 2 * 2:2], mixed[1:number_of // 2 * 2:2]
    room = jnp.minimum(sizes[donor] - 1, most - sizes[taker]) // 2
    room = jnp.where((donor == order[0]) | (taker == order[0]) | (sizes[taker] == 0), 0, jnp.maximum(room, 0))
    moved = jax.random.randint(jax.random.fold_in(own, 4), (number_of // 2,), 0, 1 << 20) % (room + 1)
    sizes = sizes.at[donor].add(-moved).at[taker].add(moved)
    members = jnp.searchsorted(jnp.cumsum(sizes), jnp.arange(rows * top), side="right").astype(jnp.int32)
    table = members.reshape(top, rows).T
    table = table[jax.random.permutation(jax.random.fold_in(own, 1), rows)]
    rotation = jax.random.randint(jax.random.fold_in(own, 2), (rows, 1), 0, top)
    return jnp.take_along_axis(table, (jnp.arange(top)[None, :] + rotation) % top, axis=1)


def load_shares(amount, total, most, lean, full):
    loads = [(1 << 20) // math.isqrt(grade ** lean) + 1 for grade in range(1, amount + 1)]
    largest = most if full else min(most, max(-(-total // amount), total * loads[0] // sum(loads)))
    least = 1 if total - largest >= amount - 1 else 0
    counts, surplus = [largest] + [least] * (amount - 1), total - largest - least * (amount - 1)
    while surplus > 0:
        free = [i for i in range(1, amount) if counts[i] < largest] or [i for i in range(1, amount) if counts[i] < most]
        pool, budget = sum([loads[i] for i in free]), surplus
        for i in free:
            more = min(most - counts[i], max(1, budget * loads[i] // pool), surplus)
            counts[i] = counts[i] + more
            surplus = surplus - more
    return np.array(counts)


def scatter_about(key, dims, scale, most, shards=(), kind=jnp.bfloat16):
    level = shard_levels(key, dims, shards, -0.22, 0.18) if shards else 1.0
    array = jax.random.normal(key, dims, jnp.float32) * scale * level
    return jnp.minimum(jnp.maximum(array, -most), most).astype(kind)


def setup_inputs(seed: int = 0) -> dict:
    seeds = jax.random.split(jax.random.key(seed), 9)
    sparse_vecs = scatter_about(seeds[0], (BATCH, TABLES, E), 1.0, 6.0, ((0, 256),))
    dense_vec = scatter_about(seeds[1], (BATCH, E), 1.0, 6.0, ((0, 256),))
    top_cot = scatter_about(seeds[2], (BATCH, H1), 0.1, 0.59765625, ((0, 256),))
    top_weight = scatter_about(seeds[3], (ZIN, H1), ZIN ** -0.5, 0.25)
    owner_ids_keys = jax.random.split(jax.random.fold_in(seeds[4], 1), BATCH * TABLES // LOOK_DEV)
    owner_ids_turns = jax.random.permutation(jax.random.fold_in(seeds[4], 3), BATCH * TABLES // LOOK_DEV)
    owner_ids = jax.vmap(lambda own, number: shared_out(jax.random.fold_in(seeds[4], 2), own, number, LOOK_DEV, N_DP, 1, CAP, 1))(owner_ids_keys, owner_ids_turns).reshape((BATCH, TABLES, 1))
    local_rows = with_ends(ranked(seeds[5], (BATCH, TABLES), ROWS_GRP, 2), jax.random.fold_in(seeds[5], 3), 0, ROWS_GRP - 1).astype(jnp.int32)
    table = scatter_about(seeds[6], (TABLES, ROWS, E), 0.1, 0.6, ((1, 256),), jnp.float32)
    accum = jnp.clip(jnp.exp(math.log(2.0) - 3.6888794 * jax.random.uniform(seeds[7], (TABLES, ROWS), jnp.float32) ** shard_levels(seeds[7], (TABLES, ROWS), ((1, 256),), -0.2, 0.2)), 0.05, 2.0)
    return dict(sparse_vecs=sparse_vecs, dense_vec=dense_vec, top_cot=top_cot, top_weight=top_weight, owner_ids=owner_ids, local_rows=local_rows, table=table, accum=accum)


LEARN_RATE = 0.1
EPSILON = 1e-08

def pair_matrix(feature_count):
    row_index, col_index = np.tril_indices(feature_count, -1)
    pair_count = row_index.shape[0]
    matrix = np.zeros((pair_count, feature_count * feature_count), np.float32)
    matrix[np.arange(pair_count), row_index * feature_count + col_index] = 1.0
    matrix[np.arange(pair_count), col_index * feature_count + row_index] = 1.0
    return matrix

def interaction(sparse_vecs, dense_vec, top_cot, top_weight):
    batch_rows, table_count, row_width = sparse_vecs.shape
    feature_count = table_count + 1
    input_cot = jnp.dot(top_cot, top_weight.T, preferred_element_type=jnp.float32)
    symmetric = jnp.dot(input_cot[:, row_width:], pair_matrix(feature_count), precision=lax.Precision.HIGHEST)
    symmetric = symmetric.reshape(batch_rows, feature_count, feature_count)
    features = jnp.concatenate([dense_vec[:, None, :], sparse_vecs], axis=1).astype(jnp.float32)
    feature_grad = jnp.einsum('bij,bje->bie', symmetric, features, precision=lax.Precision.HIGHEST)
    dense_grad = (input_cot[:, :row_width] + feature_grad[:, 0]).astype(jnp.bfloat16)
    sparse_grad = feature_grad[:, 1:].astype(jnp.bfloat16)
    return (dense_grad, sparse_grad)

def reference(sparse_vecs, dense_vec, top_cot, top_weight, owner_ids, local_rows, table, accum):
    block_count = BATCH // B_DEV

    def one_block(blocks):
        return interaction(blocks[0], blocks[1], blocks[2], top_weight)
    dense_grad, sparse_grad = lax.map(one_block, (sparse_vecs.reshape(block_count, B_DEV, TABLES, E), dense_vec.reshape(block_count, B_DEV, E), top_cot.reshape(block_count, B_DEV, H1)))
    dense_grad = dense_grad.reshape(BATCH, E)
    sparse_grad = sparse_grad.reshape(BATCH, TABLES, E)
    row_total = ROWS_GRP * N_DP
    row_keys = jnp.arange(TABLES, dtype=jnp.int32)[None, :] * row_total + owner_ids[:, :, 0] * ROWS_GRP + local_rows
    row_grad = jax.ops.segment_sum(sparse_grad.astype(jnp.float32).reshape(BATCH * TABLES, E), row_keys.reshape(BATCH * TABLES).astype(jnp.int32), num_segments=TABLES * row_total)
    row_grad = row_grad.reshape(TABLES, row_total, E)
    new_accum = accum + lax.optimization_barrier(jnp.mean(row_grad * row_grad, axis=-1))
    new_table = table - LEARN_RATE * row_grad / (jnp.sqrt(new_accum)[:, :, None] + EPSILON)
    return (dense_grad, new_table, new_accum)
```

```python
import jax
import jax.numpy as jnp
from jax import lax
from jax.experimental import pallas as pl
from jax.experimental.pallas import tpu as pltpu
from jax.sharding import PartitionSpec as P

LEARN_RATE = 0.1
EPSILON = 1e-08

MESH = pl.DeviceIdType.MESH
BF16 = jnp.bfloat16
F32 = jnp.float32
I32 = jnp.int32

BATCH = 256
TABLES = 26
FEATS = 27
WIDTH = 128
GROUP = 8
GROUPS = BATCH // GROUP
ITEMS = TABLES * GROUP
LOOKUPS = BATCH * TABLES
CAP = 208
RANKS = 256
OWNERS = 64
PIECE = 832
PIECES = 4
PLANE = 32
SLOTS = 2 * PLANE


def prepare_kernel(comb_ref, sparse_ref, dense_ref, cot_ref, weight_ref, grad_ref, dgrad_ref, src_ref, key_ref,
                   member_ref, cum_ref, sym_ref, ic_ref):
    sample = lax.broadcasted_iota(I32, (1, BATCH), 1)
    upto = (lax.broadcasted_iota(I32, (BATCH, BATCH), 0) <= lax.broadcasted_iota(I32, (BATCH, BATCH), 1)).astype(F32).astype(BF16)
    owner_row = lax.broadcasted_iota(I32, (OWNERS, BATCH), 0)
    for t in range(TABLES):
        own = lax.shift_right_logical(comb_ref[t : t + 1, :], 7)
        member_ref[t * OWNERS : (t + 1) * OWNERS, :] = (own == owner_row).astype(F32).astype(BF16)
    cum_ref[...] = jnp.dot(member_ref[...], upto, preferred_element_type=F32)
    group_of = (lax.shift_right_logical(sample, 3) + 1).astype(F32)
    rank_row = lax.broadcasted_iota(I32, (RANKS, BATCH), 0)
    carry = jnp.zeros((OWNERS, 1), F32)
    found = jnp.zeros((3 * OWNERS, RANKS), F32)
    for t in range(TABLES):
        member = member_ref[t * OWNERS : (t + 1) * OWNERS, :].astype(F32)
        count = cum_ref[t * OWNERS : (t + 1) * OWNERS, :] + carry
        rank = jnp.sum(member * count, axis=0, keepdims=True).astype(I32) - 1
        carry = count[:, BATCH - 1 : BATCH]
        at_rank = (rank == rank_row).astype(F32).astype(BF16)
        row = (comb_ref[t : t + 1, :] & 127).astype(F32)
        place = (t * GROUP + (sample & 7)).astype(F32)
        values = jnp.concatenate([member * group_of, member * place, member * row], axis=0).astype(BF16)
        found = found + lax.dot_general(values, at_rank, (((1,), (1,)), ((), ())), preferred_element_type=F32)
    found = found.astype(I32)
    group, place, row = found[:OWNERS], found[OWNERS : 2 * OWNERS], found[2 * OWNERS :]
    src_ref[...] = jnp.where(group > 0, (group - 1) * ITEMS + place, LOOKUPS)
    key_ref[...] = lax.shift_right_logical(row, 5) * PIECE + lax.shift_right_logical(place, 3) * 32 + (row & 31)

    ic = lax.dot_general(cot_ref[...], weight_ref[...], (((1,), (1,)), ((), ())), preferred_element_type=F32)
    ic_ref[...] = ic[:, :WIDTH]
    pairs = ic[:, WIDTH:].astype(BF16)
    pair_count = pairs.shape[1]
    pair_row = lax.broadcasted_iota(I32, (pair_count, 256), 0)
    lane = lax.broadcasted_iota(I32, (1, 256), 1)
    col = lane & 31
    other = jnp.where(col == FEATS - 1, 0, col + 1)
    own_sample = (lax.broadcasted_iota(I32, (GROUP, 256), 0) == lax.shift_right_logical(lax.broadcasted_iota(I32, (GROUP, 256), 1), 5))[None]

    def spread(f):
        if f >= FEATS:
            return jnp.zeros((GROUPS, GROUP, 256), F32)
        this = (f + 1) % FEATS
        low, high = jnp.minimum(other, this), jnp.maximum(other, this)
        pair = lax.shift_right_logical(high * (high - 1), 1) + low
        pair = jnp.where((col < FEATS) & (other != this), pair, -1)
        place = (pair_row == pair).astype(F32).astype(BF16)
        wide = jnp.dot(pairs, place, preferred_element_type=F32).reshape(GROUPS, GROUP, 256)
        return jnp.where(own_sample, wide, 0.0)

    for f in range(0, FEATS + 1, 2):
        sym_ref[:, f * GROUP : (f + 2) * GROUP, :] = jnp.concatenate([spread(f), spread(f + 1)], axis=1).astype(BF16)

    def one_group(g, _):
        first = pl.multiple_of(g * GROUP, GROUP)
        feats = jnp.concatenate(
            [sparse_ref[pl.ds(first, GROUP)], dense_ref[pl.ds(first, GROUP), :][:, None, :], jnp.zeros((GROUP, 32 - FEATS, WIDTH), BF16)],
            axis=1,
        ).reshape(GROUP * 32, WIDTH)
        out = jnp.dot(sym_ref[g], feats, preferred_element_type=F32)
        grad_ref[pl.ds(pl.multiple_of(g * ITEMS, 8), ITEMS), :] = out[:ITEMS]
        dgrad_ref[pl.ds(first, GROUP), :] = (ic_ref[pl.ds(first, GROUP), :] + out[ITEMS : ITEMS + GROUP]).astype(BF16)
        return 0

    lax.fori_loop(0, GROUPS, one_group, 0)
    grad_ref[LOOKUPS : LOOKUPS + 8, :] = jnp.zeros((8, WIDTH), F32)


def prepare(comb, sparse_vecs, dense_vec, top_cot, top_weight):
    vmem = pl.BlockSpec(memory_space=pltpu.VMEM)
    return pl.pallas_call(
        prepare_kernel,
        out_shape=(
            jax.ShapeDtypeStruct((LOOKUPS + 8, WIDTH), F32),
            jax.ShapeDtypeStruct((BATCH, WIDTH), BF16),
            jax.ShapeDtypeStruct((OWNERS, RANKS), I32),
            jax.ShapeDtypeStruct((OWNERS, RANKS), I32),
        ),
        in_specs=[vmem] * 5,
        out_specs=(vmem,) * 4,
        scratch_shapes=[
            pltpu.VMEM((TABLES * OWNERS, BATCH), BF16),
            pltpu.VMEM((TABLES * OWNERS, BATCH), F32),
            pltpu.VMEM((GROUPS, (FEATS + 1) * GROUP, 256), BF16),
            pltpu.VMEM((BATCH, WIDTH), F32),
        ],
        name="prepare",
    )(comb, sparse_vecs, dense_vec, top_cot, top_weight)


def shift_of(y, z, half):
    quarter = lax.rem(z - half - jnp.where(y == 3, 2, 0) + 8, 4)
    odd = jnp.where(quarter == 0, -1, jnp.where(quarter == 1, 1, jnp.where(quarter == 2, 3, -3)))
    even = jnp.where(y == 0, 4 * lax.rem(half + z // 2, 2), 2 - 4 * lax.rem(half + z, 2))
    return jnp.where(lax.rem(y, 2) == 1, odd, even)


def exchange_kernel(grad_ref, src_ref, key_ref, out_ref, rows_out, rows_in, keys_in, block, acc, piece_out, piece_in,
                    row_send, row_recv, key_send, key_recv, piece_send, piece_recv):
    dp, y = lax.axis_index("dp"), lax.axis_index("mp")
    x, z, core = dp // 16, lax.rem(dp // 2, 8), lax.rem(dp, 2)

    def dp_of(x, z, core):
        return x * 16 + z * 2 + core

    def peer(step):
        mixed = lax.rem(step * 5, PLANE)
        px, py = lax.rem(x + mixed // 8, 4), lax.rem(y + lax.rem(mixed // 2, 4), 4)
        return px, py, lax.rem(core + mixed, 2)

    def target(half):
        return lax.rem(z + shift_of(y, z, half) + 8, 8)

    barrier = pltpu.get_barrier_semaphore()

    def greet_plane(step, _):
        mixed = lax.rem(step * 5, PLANE)
        px, py = lax.rem(x - mixed // 8 + 4, 4), lax.rem(y - lax.rem(mixed // 2, 4) + 4, 4)
        pl.semaphore_signal(barrier, inc=1, device_id=(dp_of(px, z, lax.rem(core + mixed, 2)), py), device_id_type=MESH)
        return 0

    lax.fori_loop(1, PLANE, greet_plane, 0)

    def greet_source(zs, _):
        away = lax.rem(z - zs + 8, 8)
        quarter = jnp.where(away == 7, 0, jnp.where(away == 1, 1, jnp.where(away == 3, 2, 3)))
        ys = jnp.where(lax.rem(away, 4) == 0, 0, jnp.where(lax.rem(away, 2) == 0, 2, jnp.where(lax.rem(zs - quarter + 8, 4) < 2, 1, 3)))

        @pl.when((zs != z) | (ys != y))
        def _():
            pl.semaphore_signal(barrier, inc=1, device_id=(dp_of(x, zs, core), ys), device_id_type=MESH)

        return 0

    lax.fori_loop(0, 8, greet_source, 0)
    pl.semaphore_wait(barrier, PLANE - 1 + 8 - jnp.where(y == 0, 1, 0))

    def owner_of(step, half):
        px, py, pcore = peer(step)
        return dp_of(px, lax.rem(z + shift_of(py, z, half) + 8, 8), pcore)

    def key_copy(slot, owner, device):
        return pltpu.make_async_remote_copy(
            src_ref=key_ref.at[owner], dst_ref=keys_in.at[slot], send_sem=key_send, recv_sem=key_recv, device_id=device, device_id_type=MESH
        )

    def send_keys(slot, _):
        half, step = slot // PLANE, lax.rem(slot, PLANE)
        owner = owner_of(step, half)
        px, py, pcore = peer(step)

        @pl.when(step == 0)
        def _():
            pltpu.make_async_copy(key_ref.at[owner], keys_in.at[slot], key_recv).start()

        @pl.when(step != 0)
        def _():
            key_copy(slot, owner, (dp_of(px, z, pcore), py)).start()

        return 0

    lax.fori_loop(0, SLOTS, send_keys, 0)

    def send_rows(slot, _):
        half, step = slot // PLANE, lax.rem(slot, PLANE)
        owner = owner_of(step, half)
        px, py, pcore = peer(step)

        def gather(r, _):
            for k in range(16):
                at = r * 16 + k
                block[pl.ds(at, 1), :] = grad_ref[pl.ds(src_ref[owner, at], 1), :]
            return 0

        lax.fori_loop(0, CAP // 16, gather, 0)

        @pl.when(step == 0)
        def _():
            rows_in[slot] = block[...].astype(BF16)

        @pl.when(step != 0)
        def _():
            rows_out[slot] = block[...].astype(BF16)
            pltpu.make_async_remote_copy(
                src_ref=rows_out.at[slot],
                dst_ref=rows_in.at[slot],
                send_sem=row_send,
                recv_sem=row_recv.at[slot],
                device_id=(dp_of(px, z, pcore), py),
                device_id_type=MESH,
            ).start()

        return 0

    lax.fori_loop(0, SLOTS, send_rows, 0)

    pltpu.make_async_copy(keys_in, keys_in, key_recv).wait()

    row_of = lax.broadcasted_iota(I32, (PIECE, CAP), 0)

    def sum_half(half):
        acc[...] = jnp.zeros_like(acc)

        def add(turn, _):
            slots = [half * PLANE + turn * 4 + k for k in range(4)]
            for slot in slots:

                @pl.when(lax.rem(slot, PLANE) != 0)
                def _():
                    pltpu.make_async_copy(rows_in.at[slot], rows_in.at[slot], row_recv.at[slot]).wait()

            rows = [rows_in[slot] for slot in slots]
            keys = [keys_in[slot][:, :CAP] for slot in slots]
            for p in range(PIECES):
                total = acc[p]
                for k in range(4):
                    onehot = (row_of == keys[k] - p * PIECE).astype(F32).astype(BF16)
                    total = total + jnp.dot(onehot, rows[k], preferred_element_type=F32)
                acc[p] = total
            return 0

        lax.fori_loop(0, PLANE // 4, add, 0)

        zt = target(half)

        def send_piece(k, _):
            p = lax.rem(y + k + 1, PIECES)
            at = half * PIECES + p
            piece_out[at] = acc[p].astype(BF16)

            @pl.when((zt == z) & (p == y))
            def _():
                pltpu.make_async_copy(piece_out.at[at], piece_in.at[z], piece_recv.at[z]).start()

            @pl.when((zt != z) | (p != y))
            def _():
                pltpu.make_async_remote_copy(
                    src_ref=piece_out.at[at],
                    dst_ref=piece_in.at[z],
                    send_sem=piece_send,
                    recv_sem=piece_recv.at[z],
                    device_id=(dp_of(x, zt, core), p),
                    device_id_type=MESH,
                ).start()

            return 0

        lax.fori_loop(0, PIECES, send_piece, 0)

    sum_half(0)
    sum_half(1)

    def add_piece(zs, total):
        pltpu.make_async_copy(piece_in.at[zs], piece_in.at[zs], piece_recv.at[zs]).wait()
        return 0

    lax.fori_loop(0, 8, add_piece, 0)
    total = piece_in[0].astype(F32)
    for zs in range(1, 8):
        total = total + piece_in[zs].astype(F32)
    out_ref[...] = total

    def rows_left(slot, _):
        @pl.when(lax.rem(slot, PLANE) != 0)
        def _():
            pltpu.make_async_copy(rows_out.at[slot], rows_out.at[slot], row_send).wait()
            pltpu.make_async_copy(key_ref.at[0], key_ref.at[0], key_send).wait()

        return 0

    lax.fori_loop(0, SLOTS, rows_left, 0)

    def piece_left(k, _):
        pltpu.make_async_copy(piece_out.at[0], piece_out.at[0], piece_send).wait()
        return 0

    lax.fori_loop(0, 2 * PIECES - jnp.where(y == 0, 1, 0), piece_left, 0)


def exchange(grad, src, key):
    vmem = pl.BlockSpec(memory_space=pltpu.VMEM)
    return pl.pallas_call(
        exchange_kernel,
        out_shape=jax.ShapeDtypeStruct((PIECE, WIDTH), F32),
        in_specs=[vmem, pl.BlockSpec(memory_space=pltpu.SMEM), vmem],
        out_specs=vmem,
        scratch_shapes=[
            pltpu.VMEM((SLOTS, CAP, WIDTH), BF16),
            pltpu.VMEM((SLOTS, CAP, WIDTH), BF16),
            pltpu.VMEM((SLOTS, 1, RANKS), I32),
            pltpu.VMEM((CAP, WIDTH), F32),
            pltpu.VMEM((PIECES, PIECE, WIDTH), F32),
            pltpu.VMEM((2 * PIECES, PIECE, WIDTH), BF16),
            pltpu.VMEM((8, PIECE, WIDTH), BF16),
            pltpu.SemaphoreType.DMA,
            pltpu.SemaphoreType.DMA((SLOTS,)),
            pltpu.SemaphoreType.DMA,
            pltpu.SemaphoreType.DMA,
            pltpu.SemaphoreType.DMA,
            pltpu.SemaphoreType.DMA((8,)),
        ],
        compiler_params=pltpu.CompilerParams(collective_id=0, has_side_effects=True),
        name="exchange",
    )(grad, src, key.reshape(OWNERS, 1, RANKS))


def per_device(sparse_vecs, dense_vec, top_cot, top_weight, owner_ids, local_rows, table, accum):
    comb = (owner_ids[:, :, 0] * 128 + local_rows).T
    grad, dense_grad, src, key = prepare(comb, sparse_vecs, dense_vec, top_cot, top_weight)
    row_grad = exchange(grad, src, key).reshape(table.shape)
    new_accum = accum + jnp.mean(row_grad * row_grad, axis=-1)
    new_table = table - LEARN_RATE * row_grad / (jnp.sqrt(new_accum)[:, :, None] + EPSILON)
    return (dense_grad, new_table, new_accum)


def solution(mesh):
    in_specs = (
        P(("dp", "mp"), None, None),
        P(("dp", "mp"), None),
        P(("dp", "mp"), None),
        P(),
        P(("dp", "mp"), None, None),
        P(("dp", "mp"), None),
        P(None, ("dp", "mp"), None),
        P(None, ("dp", "mp")),
    )
    out_specs = (P(("dp", "mp"), None), P(None, ("dp", "mp"), None), P(None, ("dp", "mp")))
    return jax.shard_map(
        per_device, mesh=mesh, in_specs=in_specs, out_specs=out_specs, check_vma=False
    )
```

```python
import jax
import jax.numpy as jnp
from jax import lax
from jax.experimental import pallas as pl
from jax.experimental.pallas import tpu as pltpu
from jax.sharding import PartitionSpec as P

LEARN_RATE = 0.1
EPSILON = 1e-08

MESH = pl.DeviceIdType.MESH
BF16 = jnp.bfloat16
F32 = jnp.float32
I32 = jnp.int32

BATCH = 256
TABLES = 26
FEATS = 27
WIDTH = 128
GROUP = 8
GROUPS = BATCH // GROUP
ITEMS = TABLES * GROUP
LOOKUPS = BATCH * TABLES
CAP = 208
RANKS = 256
OWNERS = 64
PIECE = 832
PIECES = 4
PLANE = 32
SLOTS = 2 * PLANE


def prepare_kernel(owner_ref, local_ref, sparse_ref, dense_ref, cot_ref, weight_ref, grad_ref, dgrad_ref, src_ref, key_ref,
                   member_ref, cum_ref, sym_ref, ic_ref):
    sample = lax.broadcasted_iota(I32, (1, BATCH), 1)
    upto = (lax.broadcasted_iota(I32, (BATCH, BATCH), 0) <= lax.broadcasted_iota(I32, (BATCH, BATCH), 1)).astype(F32).astype(BF16)
    owner_row = lax.broadcasted_iota(I32, (OWNERS, BATCH), 0)
    for t in range(TABLES):
        own = owner_ref[t]
        member_ref[t * OWNERS : (t + 1) * OWNERS, :] = (own == owner_row).astype(F32).astype(BF16)
    cum_ref[...] = jnp.dot(member_ref[...], upto, preferred_element_type=F32)
    group_of = (lax.shift_right_logical(sample, 3) + 1).astype(F32)
    rank_row = lax.broadcasted_iota(I32, (RANKS, BATCH), 0)
    carry = jnp.zeros((OWNERS, 1), F32)
    found = jnp.zeros((3 * OWNERS, RANKS), F32)
    for t in range(TABLES):
        member = member_ref[t * OWNERS : (t + 1) * OWNERS, :].astype(F32)
        count = cum_ref[t * OWNERS : (t + 1) * OWNERS, :] + carry
        rank = jnp.sum(member * count, axis=0, keepdims=True).astype(I32) - 1
        carry = count[:, BATCH - 1 : BATCH]
        at_rank = (rank == rank_row).astype(F32).astype(BF16)
        row = local_ref[t : t + 1, :].astype(F32)
        place = (t * GROUP + (sample & 7)).astype(F32)
        values = jnp.concatenate([member * group_of, member * place, member * row], axis=0).astype(BF16)
        found = found + lax.dot_general(values, at_rank, (((1,), (1,)), ((), ())), preferred_element_type=F32)
    found = found.astype(I32)
    group, place, row = found[:OWNERS], found[OWNERS : 2 * OWNERS], found[2 * OWNERS :]
    src_ref[...] = jnp.where(group > 0, (group - 1) * ITEMS + place, LOOKUPS)
    key = lax.shift_right_logical(row, 5) * PIECE + lax.shift_right_logical(place, 3) * 32 + (row & 31)
    key_ref[...] = key[:, None, :]

    ic = lax.dot_general(cot_ref[...], weight_ref[...], (((1,), (1,)), ((), ())), preferred_element_type=F32)
    ic_ref[...] = ic[:, :WIDTH]
    pairs = ic[:, WIDTH:].astype(BF16)
    pair_count = pairs.shape[1]
    pair_row = lax.broadcasted_iota(I32, (pair_count, 256), 0)
    lane = lax.broadcasted_iota(I32, (1, 256), 1)
    col = lax.shift_right_logical(lane, 3)
    other = jnp.where(col == FEATS - 1, 0, col + 1)
    own_sample = (lax.broadcasted_iota(I32, (GROUP, 256), 0) == (lax.broadcasted_iota(I32, (GROUP, 256), 1) & 7))[None]

    def spread(f):
        if f >= FEATS:
            return jnp.zeros((GROUPS, GROUP, 256), F32)
        this = (f + 1) % FEATS
        low, high = jnp.minimum(other, this), jnp.maximum(other, this)
        pair = lax.shift_right_logical(high * (high - 1), 1) + low
        pair = jnp.where((col < FEATS) & (other != this), pair, -1)
        place = (pair_row == pair).astype(F32).astype(BF16)
        wide = jnp.dot(pairs, place, preferred_element_type=F32).reshape(GROUPS, GROUP, 256)
        return jnp.where(own_sample, wide, 0.0)

    for f in range(0, FEATS + 1, 2):
        sym_ref[:, f * GROUP : (f + 2) * GROUP, :] = jnp.concatenate([spread(f), spread(f + 1)], axis=1).astype(BF16)

    def one_group(g, _):
        first = pl.multiple_of(g * GROUP, GROUP)
        feats = jnp.concatenate(
            [sparse_ref[:, pl.ds(first, GROUP), :], dense_ref[pl.ds(first, GROUP), :][None], jnp.zeros((32 - FEATS, GROUP, WIDTH), BF16)],
            axis=0,
        ).reshape(GROUP * 32, WIDTH)
        out = jnp.dot(sym_ref[g], feats, preferred_element_type=F32)
        grad_ref[pl.ds(pl.multiple_of(g * ITEMS, 8), ITEMS), :] = out[:ITEMS]
        dgrad_ref[pl.ds(first, GROUP), :] = (ic_ref[pl.ds(first, GROUP), :] + out[ITEMS : ITEMS + GROUP]).astype(BF16)
        return 0

    lax.fori_loop(0, GROUPS, one_group, 0)
    grad_ref[LOOKUPS : LOOKUPS + 8, :] = jnp.zeros((8, WIDTH), F32)


def prepare(owner, local, sparse_vecs, dense_vec, top_cot, top_weight):
    vmem = pl.BlockSpec(memory_space=pltpu.VMEM)
    return pl.pallas_call(
        prepare_kernel,
        out_shape=(
            jax.ShapeDtypeStruct((LOOKUPS + 8, WIDTH), F32),
            jax.ShapeDtypeStruct((BATCH, WIDTH), BF16),
            jax.ShapeDtypeStruct((OWNERS, RANKS), I32),
            jax.ShapeDtypeStruct((OWNERS, 1, RANKS), I32),
        ),
        in_specs=[vmem] * 6,
        out_specs=(vmem,) * 4,
        scratch_shapes=[
            pltpu.VMEM((TABLES * OWNERS, BATCH), BF16),
            pltpu.VMEM((TABLES * OWNERS, BATCH), F32),
            pltpu.VMEM((GROUPS, (FEATS + 1) * GROUP, 256), BF16),
            pltpu.VMEM((BATCH, WIDTH), F32),
        ],
        name="prepare",
    )(owner, local, sparse_vecs, dense_vec, top_cot, top_weight)


def shift_of(y, z, half):
    quarter = lax.rem(z - half - jnp.where(y == 3, 2, 0) + 8, 4)
    odd = jnp.where(quarter == 0, -1, jnp.where(quarter == 1, 1, jnp.where(quarter == 2, 3, -3)))
    even = jnp.where(y == 0, 4 * lax.rem(half + z // 2, 2), 2 - 4 * lax.rem(half + z, 2))
    return jnp.where(lax.rem(y, 2) == 1, odd, even)


def exchange_kernel(grad_ref, src_ref, key_ref, out_ref, rows_out, rows_in, keys_in, block, acc, piece_out, piece_in,
                    row_send, row_recv, key_send, key_recv, piece_send, piece_recv):
    dp, y = lax.axis_index("dp"), lax.axis_index("mp")
    x, z, core = dp // 16, lax.rem(dp // 2, 8), lax.rem(dp, 2)

    def dp_of(x, z, core):
        return x * 16 + z * 2 + core

    def peer(step):
        mixed = lax.rem(step * 5, PLANE)
        px, py = lax.rem(x + mixed // 8, 4), lax.rem(y + lax.rem(mixed // 2, 4), 4)
        return px, py, lax.rem(core + mixed, 2)

    def target(half):
        return lax.rem(z + shift_of(y, z, half) + 8, 8)

    barrier = pltpu.get_barrier_semaphore()

    def greet_plane(step, _):
        mixed = lax.rem(step * 5, PLANE)
        px, py = lax.rem(x - mixed // 8 + 4, 4), lax.rem(y - lax.rem(mixed // 2, 4) + 4, 4)
        pl.semaphore_signal(barrier, inc=1, device_id=(dp_of(px, z, lax.rem(core + mixed, 2)), py), device_id_type=MESH)
        return 0

    lax.fori_loop(1, PLANE, greet_plane, 0)

    def greet_source(zs, _):
        away = lax.rem(z - zs + 8, 8)
        quarter = jnp.where(away == 7, 0, jnp.where(away == 1, 1, jnp.where(away == 3, 2, 3)))
        ys = jnp.where(lax.rem(away, 4) == 0, 0, jnp.where(lax.rem(away, 2) == 0, 2, jnp.where(lax.rem(zs - quarter + 8, 4) < 2, 1, 3)))

        @pl.when((zs != z) | (ys != y))
        def _():
            pl.semaphore_signal(barrier, inc=1, device_id=(dp_of(x, zs, core), ys), device_id_type=MESH)

        return 0

    lax.fori_loop(0, 8, greet_source, 0)
    pl.semaphore_wait(barrier, PLANE - 1 + 8 - jnp.where(y == 0, 1, 0))

    def owner_of(step, half):
        px, py, pcore = peer(step)
        return dp_of(px, lax.rem(z + shift_of(py, z, half) + 8, 8), pcore)

    def key_copy(slot, owner, device):
        return pltpu.make_async_remote_copy(
            src_ref=key_ref.at[owner], dst_ref=keys_in.at[slot], send_sem=key_send, recv_sem=key_recv, device_id=device, device_id_type=MESH
        )

    def send_keys(slot, _):
        half, step = slot // PLANE, lax.rem(slot, PLANE)
        owner = owner_of(step, half)
        px, py, pcore = peer(step)

        @pl.when(step == 0)
        def _():
            pltpu.make_async_copy(key_ref.at[owner], keys_in.at[slot], key_recv).start()

        @pl.when(step != 0)
        def _():
            key_copy(slot, owner, (dp_of(px, z, pcore), py)).start()

        return 0

    lax.fori_loop(0, SLOTS, send_keys, 0)

    def send_rows(slot, _):
        half, step = slot // PLANE, lax.rem(slot, PLANE)
        owner = owner_of(step, half)
        px, py, pcore = peer(step)

        for rank in range(CAP):
            block[rank : rank + 1, :] = grad_ref[pl.ds(src_ref[owner, rank], 1), :]

        @pl.when(step == 0)
        def _():
            rows_in[slot] = block[...].astype(BF16)

        @pl.when(step != 0)
        def _():
            rows_out[slot] = block[...].astype(BF16)
            pltpu.make_async_remote_copy(
                src_ref=rows_out.at[slot],
                dst_ref=rows_in.at[slot],
                send_sem=row_send,
                recv_sem=row_recv.at[slot],
                device_id=(dp_of(px, z, pcore), py),
                device_id_type=MESH,
            ).start()

        return 0

    lax.fori_loop(0, SLOTS, send_rows, 0)

    pltpu.make_async_copy(keys_in, keys_in, key_recv).wait()

    row_of = lax.broadcasted_iota(I32, (PIECE, CAP), 0)

    def sum_half(half):
        acc[...] = jnp.zeros_like(acc)

        def add(turn, _):
            slots = [half * PLANE + turn * 4 + k for k in range(4)]
            for slot in slots:

                @pl.when(lax.rem(slot, PLANE) != 0)
                def _():
                    pltpu.make_async_copy(rows_in.at[slot], rows_in.at[slot], row_recv.at[slot]).wait()

            total = None
            for slot in slots:
                key = keys_in[slot][:, :CAP]
                piece = sum((key >= p * PIECE).astype(I32) for p in range(1, PIECES))
                piece_col = jnp.broadcast_to(piece.astype(F32), (8, CAP)).T[:, :1]
                rows = rows_in[slot].astype(F32)
                wide = jnp.concatenate([jnp.where(piece_col == float(p), rows, 0.0).astype(BF16) for p in range(PIECES)], axis=1)
                onehot = (row_of == key - piece * PIECE).astype(F32).astype(BF16)
                part = jnp.dot(onehot, wide, preferred_element_type=F32)
                total = part if total is None else total + part
            for p in range(PIECES):
                acc[p] += total[:, p * WIDTH : (p + 1) * WIDTH]
            return 0

        lax.fori_loop(0, PLANE // 4, add, 0)

        zt = target(half)

        def send_piece(k, _):
            p = lax.rem(y + k + 1, PIECES)
            at = half * PIECES + p
            piece_out[at] = acc[p].astype(BF16)

            @pl.when((zt == z) & (p == y))
            def _():
                pltpu.make_async_copy(piece_out.at[at], piece_in.at[z], piece_recv.at[z]).start()

            @pl.when((zt != z) | (p != y))
            def _():
                pltpu.make_async_remote_copy(
                    src_ref=piece_out.at[at],
                    dst_ref=piece_in.at[z],
                    send_sem=piece_send,
                    recv_sem=piece_recv.at[z],
                    device_id=(dp_of(x, zt, core), p),
                    device_id_type=MESH,
                ).start()

            return 0

        lax.fori_loop(0, PIECES, send_piece, 0)

    sum_half(0)
    sum_half(1)

    def add_piece(zs, total):
        pltpu.make_async_copy(piece_in.at[zs], piece_in.at[zs], piece_recv.at[zs]).wait()
        return 0

    lax.fori_loop(0, 8, add_piece, 0)
    total = piece_in[0].astype(F32)
    for zs in range(1, 8):
        total = total + piece_in[zs].astype(F32)
    out_ref[...] = total

    def rows_left(slot, _):
        @pl.when(lax.rem(slot, PLANE) != 0)
        def _():
            pltpu.make_async_copy(rows_out.at[slot], rows_out.at[slot], row_send).wait()
            pltpu.make_async_copy(key_ref.at[0], key_ref.at[0], key_send).wait()

        return 0

    lax.fori_loop(0, SLOTS, rows_left, 0)

    def piece_left(k, _):
        pltpu.make_async_copy(piece_out.at[0], piece_out.at[0], piece_send).wait()
        return 0

    lax.fori_loop(0, 2 * PIECES - jnp.where(y == 0, 1, 0), piece_left, 0)


def exchange(grad, src, key):
    vmem = pl.BlockSpec(memory_space=pltpu.VMEM)
    return pl.pallas_call(
        exchange_kernel,
        out_shape=jax.ShapeDtypeStruct((PIECE, WIDTH), F32),
        in_specs=[vmem, pl.BlockSpec(memory_space=pltpu.SMEM), vmem],
        out_specs=vmem,
        scratch_shapes=[
            pltpu.VMEM((SLOTS, CAP, WIDTH), BF16),
            pltpu.VMEM((SLOTS, CAP, WIDTH), BF16),
            pltpu.VMEM((SLOTS, 1, RANKS), I32),
            pltpu.VMEM((CAP, WIDTH), F32),
            pltpu.VMEM((PIECES, PIECE, WIDTH), F32),
            pltpu.VMEM((2 * PIECES, PIECE, WIDTH), BF16),
            pltpu.VMEM((8, PIECE, WIDTH), BF16),
            pltpu.SemaphoreType.DMA,
            pltpu.SemaphoreType.DMA((SLOTS,)),
            pltpu.SemaphoreType.DMA,
            pltpu.SemaphoreType.DMA,
            pltpu.SemaphoreType.DMA,
            pltpu.SemaphoreType.DMA((8,)),
        ],
        compiler_params=pltpu.CompilerParams(collective_id=0, has_side_effects=True),
        name="exchange",
    )(grad, src, key)


def per_device(sparse_vecs, dense_vec, top_cot, top_weight, owner_ids, local_rows, table, accum):
    owner = jnp.transpose(owner_ids, (1, 2, 0))
    sparse_vecs = jnp.transpose(sparse_vecs, (1, 0, 2))
    grad, dense_grad, src, key = prepare(owner, local_rows.T, sparse_vecs, dense_vec, top_cot, top_weight)
    row_grad = exchange(grad, src, key).reshape(table.shape)
    new_accum = accum + jnp.mean(row_grad * row_grad, axis=-1)
    new_table = table - LEARN_RATE * row_grad / (jnp.sqrt(new_accum)[:, :, None] + EPSILON)
    return (dense_grad, new_table, new_accum)


def solution(mesh):
    in_specs = (
        P(("dp", "mp"), None, None),
        P(("dp", "mp"), None),
        P(("dp", "mp"), None),
        P(),
        P(("dp", "mp"), None, None),
        P(("dp", "mp"), None),
        P(None, ("dp", "mp"), None),
        P(None, ("dp", "mp")),
    )
    out_specs = (P(("dp", "mp"), None), P(None, ("dp", "mp"), None), P(None, ("dp", "mp")))
    return jax.shard_map(
        per_device, mesh=mesh, in_specs=in_specs, out_specs=out_specs, check_vma=False
    )
```
